32 devices in a mesh: rep: 16 (over z, y, x), shard: 2 (over core).
Axes of the slice: x: 2, y: 2, z: 4, core: 2. Of those that a mesh axis runs over, the one named last changes fastest.
Arguments:
- outer_params: float32 [4, 131072], P('shard'), may hold values from -6 to 6
- replica_delta: float32 [16, 4, 131072], P('rep', 'shard'), may hold values from -20 to 20
- momentum: float32 [4, 131072], P('shard', 'rep'), may hold values from -20 to 20
- tensor_of_block: int32 [4], P('shard'), may hold values from 0 to 1, as said below
Outputs:
- new_params: float32 [4, 131072], P('shard')
- new_momentum: float32 [4, 131072], P('shard', 'rep')
The draws below stay inside these ranges and needn't reach their ends.
Inputs may be any that keep to these rules, and one draw needn't show every extreme that they name: `tensor_of_block`: every tensor owns exactly 2 blocks.
All inputs are finite; a program needn't handle non-finite values.
Results may differ from the reference program's by a relative error of at most 0.00028.
Values sent between devices are 32-bit elements; how exact they have to be, the bound alone decides.
A program may use at most 64 MiB of HBM per device.

```python
import math
import jax
import jax.numpy as jnp
from jax import lax

BLOCK_ROWS = 128
BLOCK_COLS = 1024
NS_STEPS = 8
REPLICAS = 16
BLOCKS = 4
GROUPS = 2


def common_parts(key):
    base = jax.random.fold_in(key, 11)
    log_scale = jax.random.uniform(jax.random.fold_in(base, 1), (BLOCKS, 1), jnp.float32, math.log(0.5), math.log(2.0))
    shared = jnp.clip(jax.random.normal(jax.random.fold_in(base, 2), (BLOCKS, BLOCK_ROWS * BLOCK_COLS), jnp.float32), -5.0, 5.0)
    align = jax.random.uniform(jax.random.fold_in(base, 3), (BLOCKS, 1), jnp.float32, -1.0, 1.0)
    return (jnp.exp(log_scale), shared, align)


def draw_momentum(key, part):
    scale, shared, align = common_parts(key)
    noise = jnp.clip(jax.random.normal(jax.random.fold_in(key, 21), shared.shape, jnp.float32), -5.0, 5.0)
    values = 0.7 * scale * (align * shared + noise)
    return values.astype(jnp.float32)


def draw_replica_delta(key, part):
    scale, shared, align = common_parts(key)
    noise = jnp.clip(jax.random.normal(jax.random.fold_in(key, 31), (REPLICAS, BLOCKS, BLOCK_ROWS * BLOCK_COLS), jnp.float32), -5.0, 5.0)
    values = scale[None] * (shared[None] + noise)
    return values.astype(jnp.float32)


def draw_tensor_of_block(key, part):
    order = jax.random.permutation(jax.random.fold_in(key, 41), BLOCKS)
    return (order % GROUPS).astype(jnp.int32)


def block_levels(stream_key, shape, shards, least, high):
    def one(position, shards_of):
        steps = jax.random.uniform(jax.random.fold_in(jax.random.fold_in(stream_key, 6), position), (shards_of,), jnp.float32, least / len(shards), high / len(shards))
        return jnp.repeat(jnp.exp(steps), shape[position] // shards_of).reshape((-1,) + (1,) * (len(shape) - position - 1))

    factor_of = one(*shards[0])
    for cut in shards[1:]:
        factor_of = factor_of * one(*cut)
    return factor_of


def gaussian(key, extent, scale, reach, split=(), held_as=jnp.bfloat16):
    drawn = jax.random.normal(key, extent, jnp.float32) * scale
    if len(split) > 0:
        drawn = block_levels(key, extent, split, -0.22, 0.18) * drawn
    return jnp.clip(drawn, min=-reach, max=reach).astype(held_as)


def setup_inputs(seed: int = 0) -> dict:
    seeds = jax.random.split(jax.random.key(seed), 5)
    return {
        "outer_params": gaussian(seeds[0], (BLOCKS, BLOCK_ROWS * BLOCK_COLS), 1.0, 6.0, ((0, 2),), jnp.float32),
        "replica_delta": draw_replica_delta(jax.random.fold_in(seeds[4], 71), 0),
        "momentum": draw_momentum(jax.random.fold_in(seeds[4], 71), 0),
        "tensor_of_block": draw_tensor_of_block(jax.random.fold_in(seeds[4], 71), 0),
    }


outer_rate = 0.7
decay_rate = 0.9

def orthogonalize(direction):
    blocks = direction.reshape(direction.shape[0], BLOCK_ROWS, BLOCK_COLS)
    blocks = blocks / jnp.sqrt(lax.optimization_barrier(jnp.sum(blocks * blocks, axis=(1, 2), keepdims=True)) + 1.0)
    for step in range(NS_STEPS):
        square = jnp.einsum('bij,bkj->bik', blocks, blocks, precision=lax.Precision.HIGHEST)
        blocks = 1.5 * blocks - 0.5 * jnp.einsum('bik,bkj->bij', square, blocks, precision=lax.Precision.HIGHEST)
    return blocks.reshape(direction.shape[0], BLOCK_ROWS * BLOCK_COLS)

def reference(outer_params, replica_delta, momentum, tensor_of_block):
    mean_delta = lax.optimization_barrier(jnp.sum(replica_delta, axis=0)) / REPLICAS
    new_momentum = decay_rate * momentum + mean_delta
    direction = mean_delta + decay_rate * new_momentum
    update = orthogonalize(direction)
    member = (tensor_of_block[:, None] == jnp.arange(GROUPS, dtype=jnp.int32)[None, :]).astype(jnp.float32)
    per_block = jnp.stack([lax.optimization_barrier(jnp.sum(outer_params * outer_params, axis=1)), lax.optimization_barrier(jnp.sum(update * update, axis=1))], axis=1)
    tensor_sums = lax.optimization_barrier(jnp.sum(member[:, :, None] * per_block[:, None, :], axis=0))
    group_rate = outer_rate * jnp.sqrt(jnp.maximum(tensor_sums[:, 0], 1.0) / jnp.maximum(tensor_sums[:, 1], 1.0))
    block_rate = lax.optimization_barrier(jnp.sum(member * group_rate[None, :], axis=1))
    new_params = outer_params - block_rate[:, None] * update
    return (new_params, new_momentum)
```

```python
import functools

import jax
import jax.numpy as jnp
from jax import lax
from jax.experimental import pallas as pl
from jax.experimental.pallas import tpu as pltpu
from jax.sharding import PartitionSpec as P

BLOCK_ROWS = 128
BLOCK_COLS = 1024
NS_STEPS = 8
LANES = 128
VMEM_BYTES = 16 * 1024 * 1024

outer_rate = 0.7
decay_rate = 0.9


def split(a):
    high = a.astype(jnp.bfloat16)
    return high, (a - high.astype(jnp.float32)).astype(jnp.bfloat16)


def left(a):
    return jnp.concatenate(split(a), axis=1)


def right(b):
    pair = jnp.concatenate(split(b), axis=1)
    return jnp.concatenate([pair, pair], axis=0)


def mm(a, b):
    both = jnp.dot(a, b, preferred_element_type=jnp.float32)
    half = both.shape[1] // 2
    return both[:, :half] + both[:, half:]


def kernel(
    planes, peers, blocks,
    tensor_ref, delta_ref, moment_ref, params_ref,
    update_ref, params, rate_ref, new_moment_ref,
    delta, moment, first_a, first_b, send_a, send_b, second_a, second_b, reduced, third,
    direction, matrix, sums, their_sums,
    load_sem, params_sem, moment_sem,
    s1a, r1a, s1b, r1b, s2a, r2a, s2b, r2b, s3, r3,
    gs, gr, gxs, gxr, gys, gyr, fas, far, fbs, fbr, ss, sr, up_sem, down_sem,
):
    rep = lax.axis_index("rep")
    shard = lax.axis_index("shard")
    x = rep % 2
    y = (rep // 2) % 2
    z = rep // 4
    nx, ny = 1 - x, 1 - y
    x_peer = {"rep": z * 4 + y * 2 + nx}
    y_peer = {"rep": z * 4 + ny * 2 + x}
    rows = delta.shape[3]
    half = rows // 2
    top, low = pl.ds(0, half), pl.ds(half, half)

    def plane(offset):
        return (z + offset) % planes

    def z_peer(offset):
        return {"rep": plane(offset) * 4 + y * 2 + x}

    order = [(k + 1) % planes for k in range(planes)]

    loads = []
    for k, offset in enumerate(order):
        at = plane(offset)
        copy = pltpu.make_async_copy(delta_ref.at[at], delta.at[at], load_sem.at[k])
        copy.start()
        loads.append(copy)
    moment_copy = pltpu.make_async_copy(moment_ref, moment, moment_sem)
    moment_copy.start()
    cols = BLOCK_COLS // LANES
    params_copies = []
    for b in range(blocks):
        for c in range(cols):
            copy = pltpu.make_async_copy(
                params_ref.at[:, c, b], params.at[b, c], params_sem.at[b * cols + c]
            )
            copy.start()
            params_copies.append(copy)

    barrier = pltpu.get_barrier_semaphore()
    targets = [x_peer, y_peer]
    targets += [{"shard": (shard + o) % peers} for o in range(1, peers)]
    for target in targets:
        pl.semaphore_signal(barrier, inc=1, device_id=target)

    def line(step):
        return {"rep": (z + step) * 4 + y * 2 + x}

    def tell(sem, distance):
        @pl.when((z >= 1) & (z + distance < planes))
        def _():
            pl.semaphore_signal(sem[0], inc=1, device_id=line(-1))

        @pl.when((z + 1 < planes) & (z - distance >= 0))
        def _():
            pl.semaphore_signal(sem[1], inc=1, device_id=line(1))

    def hear(distance):
        @pl.when(z + 1 + distance < planes)
        def _():
            pl.semaphore_wait(up_sem.at[distance], 1)

        @pl.when(z - 1 - distance >= 0)
        def _():
            pl.semaphore_wait(down_sem.at[distance], 1)

    def relay(distance):
        tell((up_sem.at[distance], down_sem.at[distance]), distance)

    tell((barrier, barrier), 0)
    inner = (z >= 1).astype(jnp.int32) + (z + 1 < planes).astype(jnp.int32)
    pl.semaphore_wait(barrier, len(targets) + inner)
    if planes > 2:
        relay(1)

    def remote(src, dst, send, recv, target):
        copy = pltpu.make_async_remote_copy(
            src_ref=src, dst_ref=dst, send_sem=send, recv_sem=recv, device_id=target
        )
        copy.start()
        return copy

    started = []

    def stage1(k):
        at = plane(order[k])
        loads[k].wait()
        a = remote(delta.at[at, :, nx, top], first_a.at[k], s1a.at[k], r1a.at[k], x_peer)
        b = remote(delta.at[at, ny, :, low], first_b.at[k], s1b.at[k], r1b.at[k], y_peer)
        started.extend([a, b])
        return a, b

    def stage2(k, first):
        at = plane(order[k])
        first[0].wait_recv()
        send_a[k] = delta[at, ny, x, top] + first_a[k, ny]
        a = remote(send_a.at[k], second_a.at[k], s2a.at[k], r2a.at[k], y_peer)
        first[1].wait_recv()
        send_b[k] = delta[at, y, nx, low] + first_b[k, nx]
        b = remote(send_b.at[k], second_b.at[k], s2b.at[k], r2b.at[k], x_peer)
        started.extend([a, b])
        return a, b

    def stage3(k, second):
        at = plane(order[k])
        second[0].wait_recv()
        reduced[k, top] = delta[at, y, x, top] + first_a[k, y] + second_a[k]
        second[1].wait_recv()
        reduced[k, low] = delta[at, y, x, low] + first_b[k, x] + second_b[k]
        if order[k] == 0:
            return None
        c = remote(reduced.at[k], third.at[k], s3.at[k], r3.at[k], z_peer(order[k]))
        started.append(c)
        return c

    ones = {}
    twos = {}
    threes = {}
    for k in range(min(3, planes)):
        ones[k] = stage1(k)

    lane = lax.broadcasted_iota(jnp.int32, (1, LANES), 1)
    member = [(lane == tensor_ref[b]).astype(jnp.float32) for b in range(blocks)]
    for copy in params_copies:
        copy.wait()
    param_sums = jnp.zeros((1, LANES), jnp.float32)
    for b in range(blocks):
        part = params[b]
        param_sums += member[b] * jnp.sum(part * part)

    for k in range(planes):
        twos[k] = stage2(k, ones[k])
        if k + 3 < planes:
            ones[k + 3] = stage1(k + 3)
        if k == 0:
            for distance in range(1, planes - 2):
                hear(distance)
                relay(distance + 1)
        if k == 1 and planes > 2:
            hear(planes - 2)
        if k >= 1:
            threes[k - 1] = stage3(k - 1, twos[k - 1])
    threes[planes - 1] = stage3(planes - 1, twos[planes - 1])

    total = reduced[planes - 1]
    for k in range(planes - 1):
        threes[k].wait_recv()
        total = total + third[k]
    mean = total / (planes * 4)
    moment_copy.wait()
    new_moment = decay_rate * moment[...] + mean
    new_moment_ref[...] = new_moment
    direction[z, y, x] = mean + decay_rate * new_moment

    gathers = {}
    near = {}

    def spread(k):
        at = plane(-k)
        own = direction.at[at, y, x]
        a = remote(own, own, gxs.at[k], gxr.at[k], x_peer)
        b = remote(own, own, gys.at[k], gyr.at[k], y_peer)
        started.extend([a, b])
        near[k] = (a, b)

    forwards = []

    def forward(k):
        at = plane(-k)
        a, b = near[k]
        b.wait_recv()
        from_y = direction.at[at, ny, x, top]
        fa = remote(from_y, from_y, fas.at[k], far.at[k], x_peer)
        a.wait_recv()
        from_x = direction.at[at, y, nx, low]
        fb = remote(from_x, from_x, fbs.at[k], fbr.at[k], y_peer)
        started.extend([fa, fb])
        forwards.extend([fa, fb])

    own = direction.at[z, y, x]
    for k in range(1, planes):
        gathers[k] = remote(own, own, gs.at[k], gr.at[k], z_peer(k))
        started.append(gathers[k])
    spread(0)
    for k in range(1, planes):
        gathers[k].wait_recv()
        spread(k)
        forward(k - 1)
    forward(planes - 1)
    for copy in forwards:
        copy.wait_recv()

    flat = direction.reshape(planes * 4 * rows, LANES)
    eye = (
        lax.broadcasted_iota(jnp.int32, (BLOCK_ROWS, BLOCK_ROWS), 0)
        == lax.broadcasted_iota(jnp.int32, (BLOCK_ROWS, BLOCK_ROWS), 1)
    ).astype(jnp.float32)
    top_rows, low_rows = pl.ds(0, BLOCK_ROWS), pl.ds(BLOCK_ROWS, BLOCK_ROWS)

    grams, firsts, polys, scales = [], [], [], []
    for b in range(blocks):
        for c in range(cols):
            high, low_part = split(flat[pl.ds(c * blocks + b, BLOCK_ROWS, stride=cols * blocks), :])
            matrix[b, top_rows, pl.ds(c * LANES, LANES)] = high
            matrix[b, low_rows, pl.ds(c * LANES, LANES)] = low_part
    for b in range(blocks):
        whole = matrix[b]
        quads = lax.dot_general(
            whole, whole, (((1,), (1,)), ((), ())), preferred_element_type=jnp.float32
        )
        halves = quads[:BLOCK_ROWS] + quads[BLOCK_ROWS:]
        gram = halves[:, :BLOCK_ROWS] + halves[:, BLOCK_ROWS:]
        scale = 1.0 / jnp.sqrt(jnp.sum(gram * eye, keepdims=True) + 1.0)
        gram = gram * (scale * scale)
        scales.append(scale)
        grams.append(gram)
        firsts.append(gram)
        polys.append(None)
    for step in range(NS_STEPS):
        last = step == NS_STEPS - 1
        factors = [1.5 * eye - 0.5 * grams[b] for b in range(blocks)]
        rights = [right(factors[b]) for b in range(blocks)]
        halfway = [None] * blocks
        for b in range(blocks):
            if not last:
                halfway[b] = mm(left(grams[b]), rights[b])
        for b in range(blocks):
            polys[b] = factors[b] if step == 0 else mm(left(polys[b]), rights[b])
        for b in range(blocks):
            if not last:
                grams[b] = mm(left(halfway[b]), rights[b])

    update_sums = jnp.zeros((1, LANES), jnp.float32)
    scaled = []
    for b in range(blocks):
        norm = jnp.sum(mm(left(polys[b]), right(firsts[b])) * polys[b])
        update_sums += member[b] * norm
        scaled.append(left(polys[b] * scales[b]))
    sums[0:1, :] = param_sums
    sums[1:2, :] = update_sums
    exchanges = []
    for o in range(1, peers):
        copy = remote(
            sums, their_sums.at[o - 1], ss.at[o - 1], sr.at[o - 1],
            {"shard": (shard + o) % peers},
        )
        exchanges.append(copy)
        started.append(copy)
    for b in range(blocks):
        for c in range(0, cols, 2):
            high = matrix[b, top_rows, pl.ds(c * LANES, 2 * LANES)]
            low_part = matrix[b, low_rows, pl.ds(c * LANES, 2 * LANES)]
            update = jnp.dot(
                scaled[b], jnp.concatenate([high, high], axis=0),
                preferred_element_type=jnp.float32,
            ) + jnp.dot(
                scaled[b], jnp.concatenate([low_part, low_part], axis=0),
                preferred_element_type=jnp.float32,
            )
            update_ref[b, c] = update[:, :LANES]
            update_ref[b, c + 1] = update[:, LANES:]
    for o, copy in enumerate(exchanges):
        copy.wait_recv()
        param_sums = param_sums + their_sums[o, 0:1, :]
        update_sums = update_sums + their_sums[o, 1:2, :]
    rate = outer_rate * jnp.sqrt(jnp.maximum(param_sums, 1.0) / jnp.maximum(update_sums, 1.0))
    for b in range(blocks):
        block_rate = jnp.sum(member[b] * rate, keepdims=True)
        rate_ref[b] = jnp.broadcast_to(block_rate, rate_ref.shape[1:])
    for copy in started:
        copy.wait_send()


def apply(update_ref, params_ref, rate_ref, moment_ref, out_ref, new_moment_ref, staged, sems, moment_sem):
    blocks, cols = update_ref.shape[:2]
    moment_copy = pltpu.make_async_copy(moment_ref, new_moment_ref, moment_sem)
    moment_copy.start()
    copies = []
    for b in range(blocks):
        rate = rate_ref[b, 0:1, :]
        for c in range(cols):
            staged[b, c] = params_ref[b, c] - rate * update_ref[b, c]
            copy = pltpu.make_async_copy(
                staged.at[b, c], out_ref.at[:, c, b], sems.at[b * cols + c]
            )
            copy.start()
            copies.append(copy)
    for copy in copies:
        copy.wait()
    moment_copy.wait()


def interleave(array):
    blocks, width = array.shape
    tiles = array.reshape(blocks, width // LANES, LANES)
    return tiles.transpose(1, 0, 2).reshape(blocks * width // LANES, LANES)


def deinterleave(array, blocks):
    tiles = array.reshape(array.shape[0] // blocks, blocks, LANES)
    return tiles.transpose(1, 0, 2).reshape(blocks, -1)


def shards(outer_params, replica_delta, momentum, tensor_of_block):
    blocks = outer_params.shape[0]
    cols = BLOCK_COLS // LANES
    replicas = lax.axis_size("rep")
    peers = lax.axis_size("shard")
    planes = replicas // 4
    moment = interleave(momentum)
    rows = moment.shape[0]
    half = rows // 2
    delta = interleave(replica_delta[0]).reshape(planes, 2, 2, rows, LANES)
    params = interleave(outer_params).reshape(BLOCK_ROWS, cols, blocks, LANES)
    f32 = jnp.float32
    vm = pltpu.VMEM
    dma = pltpu.SemaphoreType.DMA
    tiles = (blocks, cols, BLOCK_ROWS, LANES)
    vmem = pl.BlockSpec(memory_space=pltpu.VMEM)
    hbm = pl.BlockSpec(memory_space=pltpu.HBM)
    update, held, rate, moved = pl.pallas_call(
        functools.partial(kernel, planes, peers, blocks),
        out_shape=(
            vm(tiles, f32),
            vm(tiles, f32),
            vm((blocks, 8, LANES), f32),
            vm(moment.shape, f32),
        ),
        in_specs=[pl.BlockSpec(memory_space=pltpu.SMEM), hbm, hbm, hbm],
        out_specs=(vmem, vmem, vmem, vmem),
        scratch_shapes=[
            vm(delta.shape, f32),
            vm(moment.shape, f32),
            vm((planes, 2, half, LANES), f32),
            vm((planes, 2, half, LANES), f32),
            vm((planes, half, LANES), f32),
            vm((planes, half, LANES), f32),
            vm((planes, half, LANES), f32),
            vm((planes, half, LANES), f32),
            vm((planes, rows, LANES), f32),
            vm((planes, rows, LANES), f32),
            vm(delta.shape, f32),
            vm((blocks, 2 * BLOCK_ROWS, BLOCK_COLS), jnp.bfloat16),
            vm((2, LANES), f32),
            vm((peers, 2, LANES), f32),
            dma((planes,)),
            dma((blocks * cols,)),
            dma,
        ]
        + [dma((planes,))] * 20
        + [dma((peers,))] * 2
        + [pltpu.SemaphoreType.REGULAR((planes,))] * 2,
        compiler_params=pltpu.CompilerParams(
            collective_id=0, has_side_effects=True, vmem_limit_bytes=VMEM_BYTES
        ),
    )(*(pltpu.with_memory_space_constraint(a, pltpu.HBM) for a in (tensor_of_block, delta, moment, params)))
    out, new_moment = pl.pallas_call(
        apply,
        out_shape=(
            jax.ShapeDtypeStruct(params.shape, f32),
            jax.ShapeDtypeStruct(moment.shape, f32),
        ),
        in_specs=[vmem] * 4,
        out_specs=(hbm, hbm),
        scratch_shapes=[vm(tiles, f32), dma((blocks * cols,)), dma],
        compiler_params=pltpu.CompilerParams(vmem_limit_bytes=8 * 1024 * 1024),
    )(update, held, rate, moved)
    out = out.reshape(-1, LANES)
    return deinterleave(out, blocks), deinterleave(new_moment, blocks)


def solution(mesh):
    return jax.shard_map(
        shards,
        mesh=mesh,
        in_specs=(P("shard", None), P("rep", "shard", None), P("shard", "rep"), P("shard")),
        out_specs=(P("shard", None), P("shard", "rep")),
        check_vma=False,
    )
```
